32 devices in a mesh: gz: 2 (over core), row: 4 (over y, x), col: 4 (over z).
Axes of the slice: x: 2, y: 2, z: 4, core: 2. Of those that a mesh axis runs over, the one named last changes fastest.
Arguments:
- rhs_sub: float32 [2, 3, 4, 96, 256], P('gz', None, 'row', 'col'), may hold values from -6 to 6
- rhs_top: float32 [2, 4, 96, 256], P(None, 'row', 'col'), may hold values from -6 to 6
- lower_sub: bfloat16 [2, 3, 4, 4, 256, 256], P('gz', None, 'row', 'col'), may hold values from -0.078125 to 0.078125
- lower_link: bfloat16 [2, 2, 4, 4, 256, 256], P('gz', None, 'row', 'col'), may hold values from -0.078125 to 0.078125
- lower_top: bfloat16 [1, 4, 4, 256, 256], P(None, 'row', 'col'), may hold values from -0.078125 to 0.078125
- inv_sub: bfloat16 [2, 3, 4, 256, 256], P('gz', None, 'row'), may hold values from -0.3 to 1.3
- inv_top: bfloat16 [2, 4, 256, 256], P(None, 'row'), may hold values from -0.3 to 1.3
- mask_sub: int32 [2, 3, 4, 4], P('gz', None, 'row', 'col'), may hold values 0 or 1
- mask_link: int32 [2, 2, 4, 4], P('gz', None, 'row', 'col'), may hold values 0 or 1
- mask_top: int32 [1, 4, 4], P(None, 'row', 'col'), may hold values 0 or 1
Outputs:
- sol_sub: float32 [2, 3, 4, 96, 256], P('gz', None, 'row', 'col')
- sol_top: float32 [2, 4, 96, 256], P(None, 'row', 'col')
The draws below stay inside these ranges and needn't reach their ends.
All inputs are finite; a program needn't handle non-finite values. No bound on the sum of `mask_sub` or of `mask_link` or of `mask_top` on one device may be relied on, other than what follows from the above.
Results may differ from the reference program's by a relative error of at most 0.02.
Values may be sent and summed in bfloat16 or wider, within the bound.
A program may use at most 64 MiB of HBM per device.

```python
import math
import jax
import jax.numpy as jnp
from jax import lax

B = 256
NRHS = 96
SUBL = 3
TOPL = 2
GROUPS = 2
NBL = 4
PAIRS = 3
TPAIRS = 1


def draw_inv_sub(key, part):
    block_shape = (GROUPS, SUBL, NBL, B, B)
    noise_draw = jax.random.truncated_normal(key, -4.0, 4.0, block_shape, jnp.float32)
    return (jnp.eye(B, dtype=jnp.float32) + 0.4 * noise_draw / math.sqrt(B)).astype(jnp.bfloat16)


def draw_inv_top(key, part):
    block_shape = (TOPL, NBL, B, B)
    noise_draw = jax.random.truncated_normal(key, -4.0, 4.0, block_shape, jnp.float32)
    return (jnp.eye(B, dtype=jnp.float32) + 0.4 * noise_draw / math.sqrt(B)).astype(jnp.bfloat16)


def touch_ends(values, rng, smallest, top_value):
    longest = values.shape.index(max(values.shape))
    spots = []
    for shift in (0, 1):
        where = [jax.random.randint(jax.random.fold_in(rng, axis), (), 0, length) for axis, length in enumerate(values.shape)]
        where[longest] = (where[longest] + shift) % values.shape[longest]
        spots.append(tuple(where))
    return values.at[spots[0]].set(smallest).at[spots[1]].set(top_value)


def shard_levels(key, extent, pieces, least, high):
    loudness, own = 1.0, jax.random.fold_in(key, 6)
    for axis_at, blocks in pieces:
        steps = jnp.exp(jax.random.uniform(jax.random.fold_in(own, axis_at), (blocks,), jnp.float32, least / len(pieces), high / len(pieces)))
        loudness = loudness * jnp.repeat(steps, extent[axis_at] // blocks).reshape([-1 if axis == axis_at else 1 for axis in range(len(extent))])
    return loudness


def scatter_about(rng, dims, width, reach, pieces=(), held_as=jnp.bfloat16):
    values = width * jax.random.normal(rng, dims, jnp.float32)
    if pieces:
        values = values * shard_levels(rng, dims, pieces, -0.22, 0.18)
    return jnp.clip(values, -reach, reach).astype(held_as)


def setup_inputs(seed: int = 0) -> dict:
    seeds = jax.random.split(jax.random.key(seed), 11)
    return {
        "rhs_sub": scatter_about(seeds[0], (GROUPS, SUBL, NBL, NRHS, B), 1.0, 6.0, ((0, 2), (2, 4), (3, 4)), jnp.float32),
        "rhs_top": scatter_about(seeds[1], (TOPL, NBL, NRHS, B), 1.0, 6.0, ((1, 4), (2, 4)), jnp.float32),
        "lower_sub": scatter_about(seeds[2], (GROUPS, PAIRS, NBL, NBL, B, B), (2 * B * NBL * SUBL) ** -0.5, 0.078125, ((0, 2), (2, 4), (3, 4))),
        "lower_link": scatter_about(seeds[3], (GROUPS, TOPL, NBL, NBL, B, B), (2 * B * NBL * SUBL) ** -0.5, 0.078125, ((0, 2), (2, 4), (3, 4))),
        "lower_top": scatter_about(seeds[4], (TPAIRS, NBL, NBL, B, B), (2 * B * NBL * SUBL) ** -0.5, 0.078125, ((1, 4), (2, 4))),
        "inv_sub": draw_inv_sub(jax.random.fold_in(seeds[10], 71), 0),
        "inv_top": draw_inv_top(jax.random.fold_in(seeds[10], 71), 0),
        "mask_sub": touch_ends((jax.random.randint(seeds[7], (GROUPS, PAIRS, NBL, NBL), 0, 4) < 3).astype(jnp.int32), jax.random.fold_in(seeds[7], 1), 0, 1),
        "mask_link": touch_ends((jax.random.randint(seeds[8], (GROUPS, TOPL, NBL, NBL), 0, 4) < 3).astype(jnp.int32), jax.random.fold_in(seeds[8], 1), 0, 1),
        "mask_top": touch_ends((jax.random.randint(seeds[9], (TPAIRS, NBL, NBL), 0, 4) < 3).astype(jnp.int32), jax.random.fold_in(seeds[9], 1), 0, 1),
    }


def pair_of(later_level, earlier):
    return later_level * (later_level - 1) // 2 + earlier


def to_half(values):
    return lax.optimization_barrier(values.astype(jnp.bfloat16))


def masked(blocks, pattern):
    return blocks.astype(jnp.float32) * pattern.astype(jnp.float32)[:, :, None, None]


def forward_apply(vectors, blocks, pattern):
    return jnp.einsum("jnb,ijbd->ind", vectors.astype(jnp.float32), masked(blocks, pattern))


def backward_apply(vectors, blocks, pattern):
    return jnp.einsum("knd,kjbd->jnb", vectors.astype(jnp.float32), masked(blocks, pattern))


def solve_rows(residual, inverse):
    rounded = to_half(residual).astype(jnp.float32)
    return jnp.einsum("inb,ibd->ind", rounded, inverse.astype(jnp.float32))


def solve_cols(residual, inverse):
    rounded = to_half(residual).astype(jnp.float32)
    return jnp.einsum("ind,ibd->inb", rounded, inverse.astype(jnp.float32))


def reference(rhs_sub, rhs_top, lower_sub, lower_link, lower_top, inv_sub, inv_top, mask_sub, mask_link, mask_top):
    sub_solved = []
    sub_half = []
    for group_index in range(GROUPS):
        solved_list = []
        half_list = []
        for tier_index in range(SUBL):
            partial_sum = jnp.zeros((NBL, NRHS, B), jnp.float32)
            for earlier in range(tier_index):
                pair_index = pair_of(tier_index, earlier)
                partial_sum = partial_sum + forward_apply(half_list[earlier], lower_sub[group_index, pair_index], mask_sub[group_index, pair_index])
            solved = solve_rows(rhs_sub[group_index, tier_index] - partial_sum, inv_sub[group_index, tier_index])
            solved_list.append(solved)
            half_list.append(to_half(solved))
        sub_solved.append(solved_list)
        sub_half.append(half_list)
    top_solved = []
    top_half = []
    for top_level in range(TOPL):
        partial_sum = jnp.zeros((NBL, NRHS, B), jnp.float32)
        for group_index in range(GROUPS):
            partial_sum = partial_sum + forward_apply(sub_half[group_index][SUBL - 1], lower_link[group_index, top_level], mask_link[group_index, top_level])
        for earlier in range(top_level):
            pair_index = pair_of(top_level, earlier)
            partial_sum = partial_sum + forward_apply(top_half[earlier], lower_top[pair_index], mask_top[pair_index])
        solved = solve_rows(rhs_top[top_level] - partial_sum, inv_top[top_level])
        top_solved.append(solved)
        top_half.append(to_half(solved))
    top_answer = [None] * TOPL
    top_answer_half = [None] * TOPL
    for top_level in reversed(range(TOPL)):
        partial_sum = jnp.zeros((NBL, NRHS, B), jnp.float32)
        for later_level in range(top_level + 1, TOPL):
            pair_index = pair_of(later_level, top_level)
            partial_sum = partial_sum + backward_apply(top_answer_half[later_level], lower_top[pair_index], mask_top[pair_index])
        answer = solve_cols(top_solved[top_level] - partial_sum, inv_top[top_level])
        top_answer[top_level] = answer
        top_answer_half[top_level] = to_half(answer)
    sub_answer = []
    for group_index in range(GROUPS):
        answers = [None] * SUBL
        answers_half = [None] * SUBL
        for tier_index in reversed(range(SUBL)):
            partial_sum = jnp.zeros((NBL, NRHS, B), jnp.float32)
            for later_level in range(tier_index + 1, SUBL):
                pair_index = pair_of(later_level, tier_index)
                partial_sum = partial_sum + backward_apply(answers_half[later_level], lower_sub[group_index, pair_index], mask_sub[group_index, pair_index])
            if tier_index == SUBL - 1:
                for top_level in range(TOPL):
                    partial_sum = partial_sum + backward_apply(top_answer_half[top_level], lower_link[group_index, top_level], mask_link[group_index, top_level])
            answer = solve_cols(sub_solved[group_index][tier_index] - partial_sum, inv_sub[group_index, tier_index])
            answers[tier_index] = answer
            answers_half[tier_index] = to_half(answer)
        sub_answer.append(jnp.stack(answers))
    return jnp.stack(sub_answer), jnp.stack(top_answer)
```

```python
import jax
import jax.numpy as jnp
from jax import lax
from jax.experimental import pallas as pl
from jax.experimental.pallas import tpu as pltpu
from jax.sharding import PartitionSpec as P


def forward_terms(column_vectors, blocks, pattern):
    product = jnp.einsum(
        "jnb,ijbd->ijnd", column_vectors, blocks, preferred_element_type=jnp.float32
    )
    return jnp.sum(product * pattern.astype(jnp.float32)[:, :, None, None], axis=1)


def backward_terms(row_vectors, blocks, pattern):
    product = jnp.einsum("knd,kjbd->kjnb", row_vectors, blocks, preferred_element_type=jnp.float32)
    return jnp.sum(product * pattern.astype(jnp.float32)[:, :, None, None], axis=0)


def inverse_rows(residual, inverse):
    return jnp.einsum(
        "inb,ibd->ind", residual.astype(jnp.bfloat16), inverse, preferred_element_type=jnp.float32
    )


def inverse_cols(residual, inverse):
    return jnp.einsum(
        "ind,ibd->inb", residual.astype(jnp.bfloat16), inverse, preferred_element_type=jnp.float32
    )


def own_share(values, share_cols):
    return lax.dynamic_slice_in_dim(values, lax.axis_index("col") * share_cols, share_cols, 1)


def level_solve(partial_sum, rhs_local, inverse, gate_value, across_groups):
    share_cols = rhs_local.shape[1]
    col_index = lax.axis_index("col")
    placed = lax.dynamic_update_slice_in_dim(
        jnp.zeros_like(partial_sum), rhs_local * gate_value, col_index * share_cols, 1
    )
    residual = lax.psum((placed - partial_sum).astype(jnp.bfloat16), "col").astype(jnp.float32)
    if across_groups:
        residual = lax.psum(residual.astype(jnp.bfloat16), "gz").astype(jnp.float32)
    result = inverse_rows(residual, inverse)
    return result


def column_vectors(rounded, col_blocks):
    col_index = lax.axis_index("col")
    every_block = lax.all_gather(rounded, "row", axis=0, tiled=True)
    result = lax.dynamic_slice_in_dim(every_block, col_index * col_blocks, col_blocks, 0)
    return result


def back_solve(back_part, solved_rows, inverse, share_cols):
    row_blocks = solved_rows.shape[0]
    summed = lax.psum(back_part.astype(jnp.bfloat16), "row").astype(jnp.float32)
    every_block = lax.all_gather(summed.astype(jnp.bfloat16), "col", axis=0, tiled=True).astype(
        summed.dtype
    )
    own_rows = lax.dynamic_slice_in_dim(
        every_block, lax.axis_index("row") * row_blocks, row_blocks, 0
    )
    answer = inverse_cols(solved_rows - own_rows, inverse)
    share = own_share(answer, share_cols)
    half = answer.astype(jnp.bfloat16)
    return (share, half)


def per_device(
    rhs_sub,
    rhs_top,
    lower_sub,
    lower_link,
    lower_top,
    inv_sub,
    inv_top,
    mask_sub,
    mask_link,
    mask_top,
):
    sub_levels = inv_sub.shape[1]
    top_levels = inv_top.shape[0]
    col_blocks = lower_top.shape[2]
    share_cols = rhs_top.shape[2]
    group_gate = (lax.axis_index("gz") == 0).astype(jnp.float32)
    unit_gate = jnp.float32(1.0)
    row_shape = (inv_top.shape[1], share_cols * lax.axis_size("col"), inv_top.shape[-1])
    column_shape = (col_blocks, row_shape[1], row_shape[2])
    sub_solved = []
    sub_columns = []
    for tier_index in range(sub_levels):
        partial_sum = jnp.zeros(row_shape, jnp.float32)
        for earlier in range(tier_index):
            pair_index = tier_index * (tier_index - 1) // 2 + earlier
            partial_sum = partial_sum + forward_terms(
                sub_columns[earlier], lower_sub[0, pair_index], mask_sub[0, pair_index]
            )
        solved = level_solve(
            partial_sum, rhs_sub[0, tier_index], inv_sub[0, tier_index], unit_gate, False
        )
        sub_solved.append(solved)
        sub_columns.append(column_vectors(solved.astype(jnp.bfloat16), col_blocks))
    top_solved = []
    top_columns = []
    for top_level in range(top_levels):
        partial_sum = forward_terms(
            sub_columns[sub_levels - 1], lower_link[0, top_level], mask_link[0, top_level]
        )
        for earlier in range(top_level):
            pair_index = top_level * (top_level - 1) // 2 + earlier
            partial_sum = partial_sum + group_gate * forward_terms(
                top_columns[earlier], lower_top[pair_index], mask_top[pair_index]
            )
        solved = level_solve(partial_sum, rhs_top[top_level], inv_top[top_level], group_gate, True)
        top_solved.append(solved)
        if top_level + 1 < top_levels:
            top_columns.append(column_vectors(solved.astype(jnp.bfloat16), col_blocks))
    top_share = [None] * top_levels
    top_half = [None] * top_levels
    for top_level in reversed(range(top_levels)):
        if top_level + 1 == top_levels:
            answer = inverse_cols(top_solved[top_level], inv_top[top_level])
            share = own_share(answer, share_cols)
            half = answer.astype(jnp.bfloat16)
        else:
            later_level = 1
            pair_index = later_level * (later_level - 1) // 2 + top_level
            back_part = backward_terms(
                top_half[later_level], lower_top[pair_index], mask_top[pair_index]
            )
            share, half = back_solve(
                back_part, top_solved[top_level], inv_top[top_level], share_cols
            )
        top_share[top_level] = share
        top_half[top_level] = half
    sub_share = [None] * sub_levels
    sub_half = [None] * sub_levels
    for tier_index in reversed(range(sub_levels)):
        back_part = jnp.zeros(column_shape, jnp.float32)
        for later_level in range(tier_index + 1, sub_levels):
            pair_index = later_level * (later_level - 1) // 2 + tier_index
            back_part = back_part + backward_terms(
                sub_half[later_level], lower_sub[0, pair_index], mask_sub[0, pair_index]
            )
        if tier_index == sub_levels - 1:
            for top_level in range(top_levels):
                back_part = back_part + backward_terms(
                    top_half[top_level], lower_link[0, top_level], mask_link[0, top_level]
                )
        share, half = back_solve(
            back_part, sub_solved[tier_index], inv_sub[0, tier_index], share_cols
        )
        sub_share[tier_index] = share
        sub_half[tier_index] = half
    sol_sub = jnp.stack(sub_share)[None]
    sol_top = jnp.stack(top_share)
    return (sol_sub, sol_top)


MESH = pl.DeviceIdType.MESH


def pair_of(later, earlier):
    return later * (later - 1) // 2 + earlier


def dot_nn(x, w):
    return lax.dot_general(x, w, (((1,), (0,)), ((), ())), preferred_element_type=jnp.float32)


def dot_nt(x, w):
    return lax.dot_general(x, w, (((1,), (1,)), ((), ())), preferred_element_type=jnp.float32)


def fused_kernel(
    rhs_sub,
    rhs_top,
    lower_sub,
    lower_link,
    lower_top,
    inv_sub,
    inv_top,
    mask_sub,
    mask_link,
    mask_top,
    sol_sub,
    sol_top,
    lm,
    solved,
    hout,
    hin,
    pout,
    pin,
    xout,
    xin,
    ans,
    qout,
    qin,
    h_send,
    h_recv,
    p_send,
    p_recv,
    x_send,
    x_recv,
    a_send,
    a_recv,
    q_send,
    q_recv,
):
    subl, topl = rhs_sub.shape[1], rhs_top.shape[0]
    pairs, tpairs = lower_sub.shape[1], lower_top.shape[0]
    levels = subl + topl
    n, share, width = hin.shape[1], hin.shape[2], hin.shape[3]
    g, i, j = lax.axis_index("gz"), lax.axis_index("row"), lax.axis_index("col")
    pending = []

    def put(src, dst, send_sem, recv_sem, where, remote=None):
        copy = pltpu.make_async_remote_copy(
            src_ref=src,
            dst_ref=dst,
            send_sem=send_sem,
            recv_sem=recv_sem,
            device_id=where,
            device_id_type=MESH,
        )
        pending.append((copy, remote))
        if remote is None:
            copy.start()
            return

        @pl.when(remote)
        def _():
            copy.start()

        @pl.when(jnp.logical_not(remote))
        def _():
            pltpu.make_async_copy(src, dst, recv_sem).start()

    def arrived(dst, recv_sem):
        pltpu.make_async_copy(dst, dst, recv_sem).wait()

    def wide(ref):
        return ref[...].astype(jnp.float32).reshape(n * share, width).astype(jnp.bfloat16)

    def inverse(level):
        return inv_sub[0, level, 0] if level < subl else inv_top[level - subl, 0]

    def rhs(level):
        return rhs_sub[0, level, 0] if level < subl else rhs_top[level - subl, 0]

    for unit in range(pairs + topl + tpairs):
        if unit < pairs:
            block, mask = lower_sub[0, unit, 0, 0], mask_sub[0, unit, 0, 0]
        elif unit < pairs + topl:
            block, mask = lower_link[0, unit - pairs, 0, 0], mask_link[0, unit - pairs, 0, 0]
        else:
            at = unit - pairs - topl
            block, mask = lower_top[at, 0, 0], mask_top[at, 0, 0]
        lm[unit] = (block.astype(jnp.float32) * mask.astype(jnp.float32)).astype(jnp.bfloat16)

    def earlier_units(level):
        if level < subl:
            return [(b, pair_of(level, b)) for b in range(level)]
        t = level - subl
        return [(subl - 1, pairs + t)] + [
            (subl + b, pairs + topl + pair_of(t, b)) for b in range(t)
        ]

    def later_units(level):
        if level >= subl:
            t = level - subl
            return [(subl + a, pairs + topl + pair_of(a, t)) for a in range(t + 1, topl)]
        found = [(a, pair_of(a, level)) for a in range(level + 1, subl)]
        if level == subl - 1:
            found += [(subl + t, pairs + t) for t in range(topl)]
        return found

    columns = {}
    for level in range(levels):
        residual = rhs(level)
        if level > 0:
            last = level - 1
            for c in range(n):
                arrived(hin.at[last, c], h_recv.at[last, c])
            columns[last] = wide(hin.at[last])
            part = None
            for b, unit in earlier_units(level):
                term = dot_nn(columns[b], lm[unit])
                part = term if part is None else part + term
            pout[level - 1] = part.reshape(n, share, width).astype(jnp.bfloat16)
            for d in range(1, n):
                c = lax.rem(j + d, n)
                put(
                    pout.at[level - 1, c],
                    pin.at[level - 1, j],
                    p_send.at[level - 1, d],
                    p_recv.at[level - 1, j],
                    {"col": c},
                )
            if level == subl:
                for t in range(topl):
                    term = part if t == 0 else dot_nn(columns[subl - 1], lm[pairs + t])
                    xout[:, t] = term.reshape(n, share, width).astype(jnp.bfloat16)
                for d in range(n):
                    c = lax.rem(j + d, n)
                    put(
                        xout.at[c],
                        xin.at[j],
                        x_send.at[d],
                        x_recv.at[j],
                        {"gz": 1 - g, "col": c},
                    )
            residual = residual - pout[level - 1, j].astype(jnp.float32)
            for d in range(1, n):
                c = lax.rem(j + d, n)
                arrived(pin.at[level - 1, c], p_recv.at[level - 1, c])
                residual = residual - pin[level - 1, c].astype(jnp.float32)
            if level >= subl:
                for c in range(n):
                    if level == subl:
                        arrived(xin.at[c], x_recv.at[c])
                    residual = residual - xin[c, level - subl].astype(jnp.float32)
        result = dot_nn(residual.astype(jnp.bfloat16), inverse(level))
        solved[level] = result
        if level + 1 < levels:
            hout[level] = result.astype(jnp.bfloat16)
            for d in range(n):
                put(
                    hout.at[level],
                    hin.at[level, j],
                    h_send.at[level, d],
                    h_recv.at[level, j],
                    {"row": lax.rem(i + d, n), "col": i},
                    None if d else i != j,
                )

    rows = {}
    for level in reversed(range(levels)):
        total = solved[level]
        if level + 1 < levels:
            last = level + 1
            for d in range(1, n):
                c = lax.rem(j + d, n)
                arrived(ans.at[last, c], a_recv.at[last, c])
            rows[last] = wide(ans.at[last])
            part = None
            for a, unit in later_units(level):
                term = dot_nt(rows[a], lm[unit])
                part = term if part is None else part + term
            qout[level] = part.reshape(n, share, width).astype(jnp.bfloat16)
            for d in range(n):
                c = lax.rem(j + d, n)
                put(
                    qout.at[level, c],
                    qin.at[level, i],
                    q_send.at[level, d],
                    q_recv.at[level, i],
                    {"row": j, "col": c},
                    None if d else i != j,
                )
            for k in range(n):
                arrived(qin.at[level, k], q_recv.at[level, k])
                total = total - qin[level, k].astype(jnp.float32)
        result = dot_nt(total.astype(jnp.bfloat16), inverse(level))
        if level < subl:
            sol_sub[0, level, 0] = result
        else:
            sol_top[level - subl, 0] = result
        if level > 0:
            ans[level, j] = result.astype(jnp.bfloat16)
            for d in range(1, n):
                put(
                    ans.at[level, j],
                    ans.at[level, j],
                    a_send.at[level, d],
                    a_recv.at[level, j],
                    {"col": lax.rem(j + d, n)},
                )

    for copy, remote in pending:
        if remote is None:
            copy.wait_send()
        else:

            @pl.when(remote)
            def _():
                copy.wait_send()


def fused_device(*args):
    rhs_sub, rhs_top, lower_sub, lower_link, lower_top = args[:5]
    levels = rhs_sub.shape[1] + rhs_top.shape[0]
    topl = rhs_top.shape[0]
    share, width = rhs_top.shape[2:]
    n = lax.axis_size("col")
    units = lower_sub.shape[1] + lower_link.shape[1] + lower_top.shape[0]
    half, dma = jnp.bfloat16, pltpu.SemaphoreType.DMA
    vmem = pl.BlockSpec(memory_space=pltpu.VMEM)
    smem = pl.BlockSpec(memory_space=pltpu.SMEM)
    vectors = pltpu.VMEM((levels, n, share, width), half)
    return pl.pallas_call(
        fused_kernel,
        out_shape=(
            jax.ShapeDtypeStruct(rhs_sub.shape, jnp.float32),
            jax.ShapeDtypeStruct(rhs_top.shape, jnp.float32),
        ),
        in_specs=[vmem] * 7 + [smem] * 3,
        out_specs=(vmem, vmem),
        scratch_shapes=[
            pltpu.VMEM((units, width, width), half),
            pltpu.VMEM((levels, share, width), jnp.float32),
            pltpu.VMEM((levels, share, width), half),
            vectors,
            vectors,
            vectors,
            pltpu.VMEM((n, topl, share, width), half),
            pltpu.VMEM((n, topl, share, width), half),
            vectors,
            vectors,
            vectors,
            dma((levels, n)),
            dma((levels, n)),
            dma((levels, n)),
            dma((levels, n)),
            dma((n,)),
            dma((n,)),
            dma((levels, n)),
            dma((levels, n)),
            dma((levels, n)),
            dma((levels, n)),
        ],
        compiler_params=pltpu.CompilerParams(has_side_effects=True),
    )(*args)


def choose(*args):
    rhs_top, lower_top = args[1], args[4]
    one_each = lower_top.shape[1] == 1 and lower_top.shape[2] == 1
    square = lax.axis_size("row") == lax.axis_size("col") and lax.axis_size("gz") == 2
    if one_each and square and rhs_top.shape[2] % 8 == 0 and rhs_top.shape[3] % 128 == 0:
        return fused_device(*args)
    return per_device(*args)


def solution(mesh):
    return jax.shard_map(
        choose,
        mesh=mesh,
        in_specs=(
            P("gz", None, "row", "col", None),
            P(None, "row", "col", None),
            P("gz", None, "row", "col", None, None),
            P("gz", None, "row", "col", None, None),
            P(None, "row", "col", None, None),
            P("gz", None, "row", None, None),
            P(None, "row", None, None),
            P("gz", None, "row", "col"),
            P("gz", None, "row", "col"),
            P(None, "row", "col"),
        ),
        out_specs=(P("gz", None, "row", "col", None), P(None, "row", "col", None)),
        check_vma=False,
    )
```

```python
import jax
import jax.numpy as jnp
from jax import lax
from jax.experimental import pallas as pl
from jax.experimental.pallas import tpu as pltpu
from jax.sharding import PartitionSpec as P


def forward_terms(column_vectors, blocks, pattern):
    product = jnp.einsum(
        "jnb,ijbd->ijnd", column_vectors, blocks, preferred_element_type=jnp.float32
    )
    return jnp.sum(product * pattern.astype(jnp.float32)[:, :, None, None], axis=1)


def backward_terms(row_vectors, blocks, pattern):
    product = jnp.einsum("knd,kjbd->kjnb", row_vectors, blocks, preferred_element_type=jnp.float32)
    return jnp.sum(product * pattern.astype(jnp.float32)[:, :, None, None], axis=0)


def inverse_rows(residual, inverse):
    return jnp.einsum(
        "inb,ibd->ind", residual.astype(jnp.bfloat16), inverse, preferred_element_type=jnp.float32
    )


def inverse_cols(residual, inverse):
    return jnp.einsum(
        "ind,ibd->inb", residual.astype(jnp.bfloat16), inverse, preferred_element_type=jnp.float32
    )


def own_share(values, share_cols):
    return lax.dynamic_slice_in_dim(values, lax.axis_index("col") * share_cols, share_cols, 1)


def level_solve(partial_sum, rhs_local, inverse, gate_value, across_groups):
    share_cols = rhs_local.shape[1]
    col_index = lax.axis_index("col")
    placed = lax.dynamic_update_slice_in_dim(
        jnp.zeros_like(partial_sum), rhs_local * gate_value, col_index * share_cols, 1
    )
    residual = lax.psum((placed - partial_sum).astype(jnp.bfloat16), "col").astype(jnp.float32)
    if across_groups:
        residual = lax.psum(residual.astype(jnp.bfloat16), "gz").astype(jnp.float32)
    result = inverse_rows(residual, inverse)
    return result


def column_vectors(rounded, col_blocks):
    col_index = lax.axis_index("col")
    every_block = lax.all_gather(rounded, "row", axis=0, tiled=True)
    result = lax.dynamic_slice_in_dim(every_block, col_index * col_blocks, col_blocks, 0)
    return result


def back_solve(back_part, solved_rows, inverse, share_cols):
    row_blocks = solved_rows.shape[0]
    summed = lax.psum(back_part.astype(jnp.bfloat16), "row").astype(jnp.float32)
    every_block = lax.all_gather(summed.astype(jnp.bfloat16), "col", axis=0, tiled=True).astype(
        summed.dtype
    )
    own_rows = lax.dynamic_slice_in_dim(
        every_block, lax.axis_index("row") * row_blocks, row_blocks, 0
    )
    answer = inverse_cols(solved_rows - own_rows, inverse)
    share = own_share(answer, share_cols)
    half = answer.astype(jnp.bfloat16)
    return (share, half)


def per_device(
    rhs_sub,
    rhs_top,
    lower_sub,
    lower_link,
    lower_top,
    inv_sub,
    inv_top,
    mask_sub,
    mask_link,
    mask_top,
):
    sub_levels = inv_sub.shape[1]
    top_levels = inv_top.shape[0]
    col_blocks = lower_top.shape[2]
    share_cols = rhs_top.shape[2]
    group_gate = (lax.axis_index("gz") == 0).astype(jnp.float32)
    unit_gate = jnp.float32(1.0)
    row_shape = (inv_top.shape[1], share_cols * lax.axis_size("col"), inv_top.shape[-1])
    column_shape = (col_blocks, row_shape[1], row_shape[2])
    sub_solved = []
    sub_columns = []
    for tier_index in range(sub_levels):
        partial_sum = jnp.zeros(row_shape, jnp.float32)
        for earlier in range(tier_index):
            pair_index = tier_index * (tier_index - 1) // 2 + earlier
            partial_sum = partial_sum + forward_terms(
                sub_columns[earlier], lower_sub[0, pair_index], mask_sub[0, pair_index]
            )
        solved = level_solve(
            partial_sum, rhs_sub[0, tier_index], inv_sub[0, tier_index], unit_gate, False
        )
        sub_solved.append(solved)
        sub_columns.append(column_vectors(solved.astype(jnp.bfloat16), col_blocks))
    top_solved = []
    top_columns = []
    for top_level in range(top_levels):
        partial_sum = forward_terms(
            sub_columns[sub_levels - 1], lower_link[0, top_level], mask_link[0, top_level]
        )
        for earlier in range(top_level):
            pair_index = top_level * (top_level - 1) // 2 + earlier
            partial_sum = partial_sum + group_gate * forward_terms(
                top_columns[earlier], lower_top[pair_index], mask_top[pair_index]
            )
        solved = level_solve(partial_sum, rhs_top[top_level], inv_top[top_level], group_gate, True)
        top_solved.append(solved)
        if top_level + 1 < top_levels:
            top_columns.append(column_vectors(solved.astype(jnp.bfloat16), col_blocks))
    top_share = [None] * top_levels
    top_half = [None] * top_levels
    for top_level in reversed(range(top_levels)):
        if top_level + 1 == top_levels:
            answer = inverse_cols(top_solved[top_level], inv_top[top_level])
            share = own_share(answer, share_cols)
            half = answer.astype(jnp.bfloat16)
        else:
            later_level = 1
            pair_index = later_level * (later_level - 1) // 2 + top_level
            back_part = backward_terms(
                top_half[later_level], lower_top[pair_index], mask_top[pair_index]
            )
            share, half = back_solve(
                back_part, top_solved[top_level], inv_top[top_level], share_cols
            )
        top_share[top_level] = share
        top_half[top_level] = half
    sub_share = [None] * sub_levels
    sub_half = [None] * sub_levels
    for tier_index in reversed(range(sub_levels)):
        back_part = jnp.zeros(column_shape, jnp.float32)
        for later_level in range(tier_index + 1, sub_levels):
            pair_index = later_level * (later_level - 1) // 2 + tier_index
            back_part = back_part + backward_terms(
                sub_half[later_level], lower_sub[0, pair_index], mask_sub[0, pair_index]
            )
        if tier_index == sub_levels - 1:
            for top_level in range(top_levels):
                back_part = back_part + backward_terms(
                    top_half[top_level], lower_link[0, top_level], mask_link[0, top_level]
                )
        share, half = back_solve(
            back_part, sub_solved[tier_index], inv_sub[0, tier_index], share_cols
        )
        sub_share[tier_index] = share
        sub_half[tier_index] = half
    sol_sub = jnp.stack(sub_share)[None]
    sol_top = jnp.stack(top_share)
    return (sol_sub, sol_top)


MESH = pl.DeviceIdType.MESH


def pair_of(later, earlier):
    return later * (later - 1) // 2 + earlier


def dot_nn(x, w):
    return lax.dot_general(x, w, (((1,), (0,)), ((), ())), preferred_element_type=jnp.float32)


def dot_nt(x, w):
    return lax.dot_general(x, w, (((1,), (1,)), ((), ())), preferred_element_type=jnp.float32)


def fused_kernel(
    rhs_sub,
    rhs_top,
    lower_sub,
    lower_link,
    lower_top,
    inv_sub,
    inv_top,
    mask,
    sol_sub,
    sol_top,
    lm,
    first,
    solved,
    hout0,
    hin0,
    qout0,
    qin0,
    rin_sub,
    rin_top,
    hout,
    hin,
    pout,
    pin,
    xout,
    xin,
    ans,
    qout,
    qin,
    back_out,
    back_in,
    r_send,
    r_recv,
    h_send,
    h_recv,
    p_send,
    p_recv,
    x_send,
    x_recv,
    a_send,
    a_recv,
    q_send,
    q_recv,
    b_send,
    b_recv,
):
    subl, topl = rhs_sub.shape[1], rhs_top.shape[0]
    pairs, tpairs = lower_sub.shape[1], lower_top.shape[0]
    levels = subl + topl
    n, share, width = hin0.shape
    mids, wide_share = hin.shape[1], hin.shape[2]
    per_mid = n // mids
    low = (n - mids) // 2
    g, i, j = lax.axis_index("gz"), lax.axis_index("row"), lax.axis_index("col")
    is_mid = (j >= low) & (j < low + mids)
    m = jnp.clip(j - low, 0, mids - 1)
    pending = []

    def put(src, dst, send_sem, recv_sem, where, remote=None, active=None):
        copy = pltpu.make_async_remote_copy(
            src_ref=src,
            dst_ref=dst,
            send_sem=send_sem,
            recv_sem=recv_sem,
            device_id=where,
            device_id_type=MESH,
        )
        goes = active
        if remote is not None:
            goes = remote if active is None else remote & active
            stays = jnp.logical_not(remote)
            stays = stays if active is None else stays & active

            @pl.when(stays)
            def _():
                pltpu.make_async_copy(src, dst, recv_sem).start()

        pending.append((copy, goes))
        if goes is None:
            copy.start()
        else:

            @pl.when(goes)
            def _():
                copy.start()

    def arrived(dst, recv_sem):
        pltpu.make_async_copy(dst, dst, recv_sem).wait()

    def inverse(level):
        return inv_sub[0, level, 0] if level < subl else inv_top[level - subl, 0]

    def rhs(level):
        if level < subl:
            value = rin_sub[:, level - 1]
        else:
            value = rin_top[:, level - subl]
        return value.reshape(wide_share, width)

    def earlier_units(level):
        if level < subl:
            return [(b, pair_of(level, b)) for b in range(level)]
        t = level - subl
        return [(subl - 1, pairs + t)] + [
            (subl + b, pairs + topl + pair_of(t, b)) for b in range(t)
        ]

    def later_units(level):
        if level >= subl:
            t = level - subl
            return [(subl + a, pairs + topl + pair_of(a, t)) for a in range(t + 1, topl)]
        found = [(a, pair_of(a, level)) for a in range(level + 1, subl)]
        if level == subl - 1:
            found += [(subl + t, pairs + t) for t in range(topl)]
        return found

    result = dot_nn(rhs_sub[0, 0, 0].astype(jnp.bfloat16), inverse(0))
    first[...] = result
    hout0[...] = result.astype(jnp.bfloat16)
    for d in range(n):
        put(
            hout0,
            hin0.at[j],
            h_send.at[0, d],
            h_recv.at[0, j],
            {"row": lax.rem(i + d, n), "col": i},
            None if d else i != j,
        )
    mid_of = low + j // per_mid
    slot = lax.rem(j, per_mid)
    for at, (src, dst) in enumerate(
        ((rhs_sub.at[0, 1:, 0], rin_sub.at[slot]), (rhs_top.at[:, 0], rin_top.at[slot]))
    ):
        put(src, dst, r_send.at[at], r_recv.at[at, slot], {"col": mid_of}, j != mid_of)

    for unit in range(pairs + topl + tpairs):
        if unit < pairs:
            block = lower_sub[0, unit, 0, 0]
        elif unit < pairs + topl:
            block = lower_link[0, unit - pairs, 0, 0]
        else:
            block = lower_top[unit - pairs - topl, 0, 0]
        gate = mask[unit].astype(jnp.float32)
        lm[unit] = (block.astype(jnp.float32) * gate).astype(jnp.bfloat16)

    columns = {}
    for level in range(1, levels):
        last = level - 1
        part = None
        for b, unit in sorted(earlier_units(level)):
            if b == last:
                if b == 0:
                    for c in range(n):
                        arrived(hin0.at[c], h_recv.at[0, c])
                    value = hin0[...].astype(jnp.float32).reshape(n * share, width)
                    columns[b] = value.astype(jnp.bfloat16)
                else:
                    for q in range(mids):
                        arrived(hin.at[b, q], h_recv.at[b, low + q])
                    columns[b] = hin[b].reshape(n * share, width)
            term = dot_nn(columns[b], lm[unit])
            part = term if part is None else part + term
        pout[level] = part.reshape(mids, wide_share, width).astype(jnp.bfloat16)
        for q in range(mids):
            put(
                pout.at[level, q],
                pin.at[level, j],
                p_send.at[level, q],
                p_recv.at[level, j],
                {"col": low + q},
                j != low + q,
            )
        if level == subl:
            for t in range(topl):
                term = part if t == 0 else dot_nn(columns[subl - 1], lm[pairs + t])
                xout[:, t] = term.reshape(mids, wide_share, width).astype(jnp.bfloat16)
            for q in range(mids):
                put(
                    xout.at[q],
                    xin.at[j],
                    x_send.at[q],
                    x_recv.at[j],
                    {"gz": 1 - g, "col": low + q},
                )

        @pl.when(is_mid)
        def _():
            if level == 1:
                for at, ref in enumerate((rin_sub, rin_top)):
                    for k in range(per_mid):
                        arrived(ref.at[k], r_recv.at[at, k])
            residual = rhs(level)
            for c in range(n):
                arrived(pin.at[level, c], p_recv.at[level, c])
                residual = residual - pin[level, c].astype(jnp.float32)
            if level >= subl:
                for c in range(n):
                    if level == subl:
                        arrived(xin.at[c], x_recv.at[c])
                    residual = residual - xin[c, level - subl].astype(jnp.float32)
            result = dot_nn(residual.astype(jnp.bfloat16), inverse(level))
            solved[level] = result
            hout[level] = result.astype(jnp.bfloat16)

        if level + 1 < levels:
            for d in range(n):
                put(
                    hout.at[level],
                    hin.at[level, m],
                    h_send.at[level, d],
                    h_recv.at[level, j],
                    {"row": lax.rem(i + d, n), "col": i},
                    None if d else i != j,
                    is_mid,
                )

    rows = {}
    for level in reversed(range(levels)):
        if level + 1 < levels:
            last = level + 1
            part = None
            for a, unit in sorted(later_units(level), reverse=True):
                if a == last:
                    for q in range(mids):

                        @pl.when(j != low + q)
                        def _():
                            arrived(ans.at[a, q], a_recv.at[a, q])

                    rows[a] = ans[a].reshape(n * share, width)
                term = dot_nt(rows[a], lm[unit])
                part = term if part is None else part + term
            if level > 0:
                qout[level] = part.reshape(mids, wide_share, width).astype(jnp.bfloat16)
                for q in range(mids):
                    put(
                        qout.at[level, q],
                        qin.at[level, i],
                        q_send.at[level, q],
                        q_recv.at[level, i],
                        {"row": j, "col": low + q},
                        (i != j) | (j != low + q),
                    )
            else:
                qout0[...] = part.reshape(n, share, width).astype(jnp.bfloat16)
                for d in range(n):
                    c = lax.rem(j + d, n)
                    put(
                        qout0.at[c],
                        qin0.at[i],
                        q_send.at[0, d],
                        q_recv.at[0, i],
                        {"row": j, "col": c},
                        None if d else i != j,
                    )
        if level == 0:
            break

        @pl.when(is_mid)
        def _():
            total = solved[level]
            if level + 1 < levels:
                for k in range(n):
                    arrived(qin.at[level, k], q_recv.at[level, k])
                    total = total - qin[level, k].astype(jnp.float32)
            result = dot_nt(total.astype(jnp.bfloat16), inverse(level))
            ans[level, m] = result.astype(jnp.bfloat16)
            back_out[level] = result.reshape(per_mid, share, width)

        for d in range(1, n):
            put(
                ans.at[level, m],
                ans.at[level, m],
                a_send.at[level, d],
                a_recv.at[level, m],
                {"col": lax.rem(j + d, n)},
                None,
                is_mid,
            )
        for k in range(per_mid):
            owner = per_mid * m + k
            put(
                back_out.at[level, k],
                back_in.at[level],
                b_send.at[level, k],
                b_recv.at[level],
                {"col": owner},
                owner != j,
                is_mid,
            )

    for level in range(1, levels):
        arrived(back_in.at[level], b_recv.at[level])
        if level < subl:
            sol_sub[0, level, 0] = back_in[level]
        else:
            sol_top[level - subl, 0] = back_in[level]
    total = first[...]
    for k in range(n):
        arrived(qin0.at[k], q_recv.at[0, k])
        total = total - qin0[k].astype(jnp.float32)
    sol_sub[0, 0, 0] = dot_nt(total.astype(jnp.bfloat16), inverse(0))

    for copy, goes in pending:
        if goes is None:
            copy.wait_send()
        else:

            @pl.when(goes)
            def _():
                copy.wait_send()


def fused_device(*args):
    rhs_sub, rhs_top, lower_sub, lower_link, lower_top = args[:5]
    subl, topl = rhs_sub.shape[1], rhs_top.shape[0]
    levels = subl + topl
    share, width = rhs_top.shape[2:]
    n = lax.axis_size("col")
    mids = n // 2
    wide_share = 2 * share
    units = lower_sub.shape[1] + lower_link.shape[1] + lower_top.shape[0]
    half, full, dma = jnp.bfloat16, jnp.float32, pltpu.SemaphoreType.DMA
    vmem = pl.BlockSpec(memory_space=pltpu.VMEM)
    smem = pl.BlockSpec(memory_space=pltpu.SMEM)

    def buffer(dtype, *shape):
        return pltpu.VMEM(shape + (width,), dtype)

    masks = jnp.concatenate([value.reshape(-1) for value in args[7:]])
    return pl.pallas_call(
        fused_kernel,
        out_shape=(
            jax.ShapeDtypeStruct(rhs_sub.shape, full),
            jax.ShapeDtypeStruct(rhs_top.shape, full),
        ),
        in_specs=[vmem] * 7 + [smem],
        out_specs=(vmem, vmem),
        scratch_shapes=[
            buffer(half, units, width),
            buffer(full, share),
            buffer(full, levels, wide_share),
            buffer(half, share),
            buffer(half, n, share),
            buffer(half, n, share),
            buffer(half, n, share),
            buffer(full, 2, subl - 1, share),
            buffer(full, 2, topl, share),
            buffer(half, levels, wide_share),
            buffer(half, levels, mids, wide_share),
            buffer(half, levels, mids, wide_share),
            buffer(half, levels, n, wide_share),
            buffer(half, mids, topl, wide_share),
            buffer(half, n, topl, wide_share),
            buffer(half, levels, mids, wide_share),
            buffer(half, levels, mids, wide_share),
            buffer(half, levels, n, wide_share),
            buffer(full, levels, 2, share),
            buffer(full, levels, share),
            dma((2,)),
            dma((2, 2)),
            dma((levels, n)),
            dma((levels, n)),
            dma((levels, n)),
            dma((levels, n)),
            dma((mids,)),
            dma((n,)),
            dma((levels, n)),
            dma((levels, mids)),
            dma((levels, n)),
            dma((levels, n)),
            dma((levels, 2)),
            dma((levels,)),
        ],
        compiler_params=pltpu.CompilerParams(has_side_effects=True),
    )(*args[:7], masks)


def choose(*args):
    rhs_top, lower_top = args[1], args[4]
    one_each = args[0].shape[1] > 1 and lower_top.shape[1] == 1 and lower_top.shape[2] == 1
    square = lax.axis_size("row") == lax.axis_size("col") and lax.axis_size("gz") == 2
    if one_each and square and rhs_top.shape[2] % 8 == 0 and lax.axis_size("col") % 4 == 0 and rhs_top.shape[3] % 128 == 0:
        return fused_device(*args)
    return per_device(*args)


def solution(mesh):
    return jax.shard_map(
        choose,
        mesh=mesh,
        in_specs=(
            P("gz", None, "row", "col", None),
            P(None, "row", "col", None),
            P("gz", None, "row", "col", None, None),
            P("gz", None, "row", "col", None, None),
            P(None, "row", "col", None, None),
            P("gz", None, "row", None, None),
            P(None, "row", None, None),
            P("gz", None, "row", "col"),
            P("gz", None, "row", "col"),
            P(None, "row", "col"),
        ),
        out_specs=(P("gz", None, "row", "col", None), P(None, "row", "col", None)),
        check_vma=False,
    )
```

```python
import jax
import jax.numpy as jnp
from jax import lax
from jax.experimental import pallas as pl
from jax.experimental.pallas import tpu as pltpu
from jax.sharding import PartitionSpec as P


def forward_terms(column_vectors, blocks, pattern):
    product = jnp.einsum(
        "jnb,ijbd->ijnd", column_vectors, blocks, preferred_element_type=jnp.float32
    )
    return jnp.sum(product * pattern.astype(jnp.float32)[:, :, None, None], axis=1)


def backward_terms(row_vectors, blocks, pattern):
    product = jnp.einsum("knd,kjbd->kjnb", row_vectors, blocks, preferred_element_type=jnp.float32)
    return jnp.sum(product * pattern.astype(jnp.float32)[:, :, None, None], axis=0)


def inverse_rows(residual, inverse):
    return jnp.einsum(
        "inb,ibd->ind", residual.astype(jnp.bfloat16), inverse, preferred_element_type=jnp.float32
    )


def inverse_cols(residual, inverse):
    return jnp.einsum(
        "ind,ibd->inb", residual.astype(jnp.bfloat16), inverse, preferred_element_type=jnp.float32
    )


def own_share(values, share_cols):
    return lax.dynamic_slice_in_dim(values, lax.axis_index("col") * share_cols, share_cols, 1)


def level_solve(partial_sum, rhs_local, inverse, gate_value, across_groups):
    share_cols = rhs_local.shape[1]
    col_index = lax.axis_index("col")
    placed = lax.dynamic_update_slice_in_dim(
        jnp.zeros_like(partial_sum), rhs_local * gate_value, col_index * share_cols, 1
    )
    residual = lax.psum((placed - partial_sum).astype(jnp.bfloat16), "col").astype(jnp.float32)
    if across_groups:
        residual = lax.psum(residual.astype(jnp.bfloat16), "gz").astype(jnp.float32)
    result = inverse_rows(residual, inverse)
    return result


def column_vectors(rounded, col_blocks):
    col_index = lax.axis_index("col")
    every_block = lax.all_gather(rounded, "row", axis=0, tiled=True)
    result = lax.dynamic_slice_in_dim(every_block, col_index * col_blocks, col_blocks, 0)
    return result


def back_solve(back_part, solved_rows, inverse, share_cols):
    row_blocks = solved_rows.shape[0]
    summed = lax.psum(back_part.astype(jnp.bfloat16), "row").astype(jnp.float32)
    every_block = lax.all_gather(summed.astype(jnp.bfloat16), "col", axis=0, tiled=True).astype(
        summed.dtype
    )
    own_rows = lax.dynamic_slice_in_dim(
        every_block, lax.axis_index("row") * row_blocks, row_blocks, 0
    )
    answer = inverse_cols(solved_rows - own_rows, inverse)
    share = own_share(answer, share_cols)
    half = answer.astype(jnp.bfloat16)
    return (share, half)


def per_device(
    rhs_sub,
    rhs_top,
    lower_sub,
    lower_link,
    lower_top,
    inv_sub,
    inv_top,
    mask_sub,
    mask_link,
    mask_top,
):
    sub_levels = inv_sub.shape[1]
    top_levels = inv_top.shape[0]
    col_blocks = lower_top.shape[2]
    share_cols = rhs_top.shape[2]
    group_gate = (lax.axis_index("gz") == 0).astype(jnp.float32)
    unit_gate = jnp.float32(1.0)
    row_shape = (inv_top.shape[1], share_cols * lax.axis_size("col"), inv_top.shape[-1])
    column_shape = (col_blocks, row_shape[1], row_shape[2])
    sub_solved = []
    sub_columns = []
    for tier_index in range(sub_levels):
        partial_sum = jnp.zeros(row_shape, jnp.float32)
        for earlier in range(tier_index):
            pair_index = tier_index * (tier_index - 1) // 2 + earlier
            partial_sum = partial_sum + forward_terms(
                sub_columns[earlier], lower_sub[0, pair_index], mask_sub[0, pair_index]
            )
        solved = level_solve(
            partial_sum, rhs_sub[0, tier_index], inv_sub[0, tier_index], unit_gate, False
        )
        sub_solved.append(solved)
        sub_columns.append(column_vectors(solved.astype(jnp.bfloat16), col_blocks))
    top_solved = []
    top_columns = []
    for top_level in range(top_levels):
        partial_sum = forward_terms(
            sub_columns[sub_levels - 1], lower_link[0, top_level], mask_link[0, top_level]
        )
        for earlier in range(top_level):
            pair_index = top_level * (top_level - 1) // 2 + earlier
            partial_sum = partial_sum + group_gate * forward_terms(
                top_columns[earlier], lower_top[pair_index], mask_top[pair_index]
            )
        solved = level_solve(partial_sum, rhs_top[top_level], inv_top[top_level], group_gate, True)
        top_solved.append(solved)
        if top_level + 1 < top_levels:
            top_columns.append(column_vectors(solved.astype(jnp.bfloat16), col_blocks))
    top_share = [None] * top_levels
    top_half = [None] * top_levels
    for top_level in reversed(range(top_levels)):
        if top_level + 1 == top_levels:
            answer = inverse_cols(top_solved[top_level], inv_top[top_level])
            share = own_share(answer, share_cols)
            half = answer.astype(jnp.bfloat16)
        else:
            later_level = 1
            pair_index = later_level * (later_level - 1) // 2 + top_level
            back_part = backward_terms(
                top_half[later_level], lower_top[pair_index], mask_top[pair_index]
            )
            share, half = back_solve(
                back_part, top_solved[top_level], inv_top[top_level], share_cols
            )
        top_share[top_level] = share
        top_half[top_level] = half
    sub_share = [None] * sub_levels
    sub_half = [None] * sub_levels
    for tier_index in reversed(range(sub_levels)):
        back_part = jnp.zeros(column_shape, jnp.float32)
        for later_level in range(tier_index + 1, sub_levels):
            pair_index = later_level * (later_level - 1) // 2 + tier_index
            back_part = back_part + backward_terms(
                sub_half[later_level], lower_sub[0, pair_index], mask_sub[0, pair_index]
            )
        if tier_index == sub_levels - 1:
            for top_level in range(top_levels):
                back_part = back_part + backward_terms(
                    top_half[top_level], lower_link[0, top_level], mask_link[0, top_level]
                )
        share, half = back_solve(
            back_part, sub_solved[tier_index], inv_sub[0, tier_index], share_cols
        )
        sub_share[tier_index] = share
        sub_half[tier_index] = half
    sol_sub = jnp.stack(sub_share)[None]
    sol_top = jnp.stack(top_share)
    return (sol_sub, sol_top)


MESH = pl.DeviceIdType.MESH


def pair_of(later, earlier):
    return later * (later - 1) // 2 + earlier


def dot_nn(x, w):
    return lax.dot_general(x, w, (((1,), (0,)), ((), ())), preferred_element_type=jnp.float32)


def dot_nt(x, w):
    return lax.dot_general(x, w, (((1,), (1,)), ((), ())), preferred_element_type=jnp.float32)


def fused_kernel(
    rhs_sub,
    rhs_top,
    lower_sub,
    lower_link,
    lower_top,
    inv_sub,
    inv_top,
    mask,
    sol_sub,
    sol_top,
    lm,
    solved,
    hout,
    hin,
    pout,
    pin,
    xout,
    xin,
    ans,
    qout,
    qin,
    h_send,
    h_recv,
    p_send,
    p_recv,
    x_send,
    x_recv,
    a_send,
    a_recv,
    q_send,
    q_recv,
):
    subl, topl = rhs_sub.shape[1], rhs_top.shape[0]
    pairs, tpairs = lower_sub.shape[1], lower_top.shape[0]
    levels = subl + topl
    n, share, width = hin.shape[1], hin.shape[2], hin.shape[3]
    g, i, j = lax.axis_index("gz"), lax.axis_index("row"), lax.axis_index("col")
    pending = []

    def put(src, dst, send_sem, recv_sem, where, remote=None):
        copy = pltpu.make_async_remote_copy(
            src_ref=src,
            dst_ref=dst,
            send_sem=send_sem,
            recv_sem=recv_sem,
            device_id=where,
            device_id_type=MESH,
        )
        pending.append((copy, remote))
        if remote is None:
            copy.start()
            return

        @pl.when(remote)
        def _():
            copy.start()

        @pl.when(jnp.logical_not(remote))
        def _():
            pltpu.make_async_copy(src, dst, recv_sem).start()

    def arrived(dst, recv_sem):
        pltpu.make_async_copy(dst, dst, recv_sem).wait()

    def wide(ref):
        return ref[...].astype(jnp.float32).reshape(n * share, width).astype(jnp.bfloat16)

    def inverse(level):
        return inv_sub[0, level, 0] if level < subl else inv_top[level - subl, 0]

    def rhs(level):
        return rhs_sub[0, level, 0] if level < subl else rhs_top[level - subl, 0]

    def mask_blocks():
        for unit in range(pairs + topl + tpairs):
            if unit < pairs:
                block = lower_sub[0, unit, 0, 0]
            elif unit < pairs + topl:
                block = lower_link[0, unit - pairs, 0, 0]
            else:
                block = lower_top[unit - pairs - topl, 0, 0]
            gate = mask[unit].astype(jnp.float32)
            lm[unit] = (block.astype(jnp.float32) * gate).astype(jnp.bfloat16)

    def earlier_units(level):
        if level < subl:
            return [(b, pair_of(level, b)) for b in range(level)]
        t = level - subl
        return [(subl - 1, pairs + t)] + [
            (subl + b, pairs + topl + pair_of(t, b)) for b in range(t)
        ]

    def later_units(level):
        if level >= subl:
            t = level - subl
            return [(subl + a, pairs + topl + pair_of(a, t)) for a in range(t + 1, topl)]
        found = [(a, pair_of(a, level)) for a in range(level + 1, subl)]
        if level == subl - 1:
            found += [(subl + t, pairs + t) for t in range(topl)]
        return found

    columns = {}
    for level in range(levels):
        residual = rhs(level)
        if level > 0:
            last = level - 1
            part = None
            for b, unit in sorted(earlier_units(level)):
                if b == last:
                    for c in range(n):
                        arrived(hin.at[last, c], h_recv.at[last, c])
                    columns[last] = wide(hin.at[last])
                term = dot_nn(columns[b], lm[unit])
                part = term if part is None else part + term
            pout[level - 1] = part.reshape(n, share, width).astype(jnp.bfloat16)
            for d in range(1, n):
                c = lax.rem(j + d, n)
                put(
                    pout.at[level - 1, c],
                    pin.at[level - 1, j],
                    p_send.at[level - 1, d],
                    p_recv.at[level - 1, j],
                    {"col": c},
                )
            if level == subl:
                for t in range(topl):
                    term = part if t == 0 else dot_nn(columns[subl - 1], lm[pairs + t])
                    xout[:, t] = term.reshape(n, share, width).astype(jnp.bfloat16)
                for d in range(n):
                    c = lax.rem(j + d, n)
                    put(
                        xout.at[c],
                        xin.at[j],
                        x_send.at[d],
                        x_recv.at[j],
                        {"gz": 1 - g, "col": c},
                    )
            residual = residual - pout[level - 1, j].astype(jnp.float32)
            for d in range(1, n):
                c = lax.rem(j + d, n)
                arrived(pin.at[level - 1, c], p_recv.at[level - 1, c])
                residual = residual - pin[level - 1, c].astype(jnp.float32)
            if level >= subl:
                for c in range(n):
                    if level == subl:
                        arrived(xin.at[c], x_recv.at[c])
                    residual = residual - xin[c, level - subl].astype(jnp.float32)
        result = dot_nn(residual.astype(jnp.bfloat16), inverse(level))
        solved[level] = result
        if level + 1 < levels:
            hout[level] = result.astype(jnp.bfloat16)
            for d in range(n):
                put(
                    hout.at[level],
                    hin.at[level, j],
                    h_send.at[level, d],
                    h_recv.at[level, j],
                    {"row": lax.rem(i + d, n), "col": i},
                    None if d else i != j,
                )
        if level == 0:
            mask_blocks()

    rows = {}
    for level in reversed(range(levels)):
        total = solved[level]
        if level + 1 < levels:
            last = level + 1
            part = None
            for a, unit in sorted(later_units(level), reverse=True):
                if a == last:
                    for d in range(1, n):
                        c = lax.rem(j + d, n)
                        arrived(ans.at[last, c], a_recv.at[last, c])
                    rows[last] = wide(ans.at[last])
                term = dot_nt(rows[a], lm[unit])
                part = term if part is None else part + term
            qout[level] = part.reshape(n, share, width).astype(jnp.bfloat16)
            for d in range(n):
                c = lax.rem(j + d, n)
                put(
                    qout.at[level, c],
                    qin.at[level, i],
                    q_send.at[level, d],
                    q_recv.at[level, i],
                    {"row": j, "col": c},
                    None if d else i != j,
                )
            for k in range(n):
                arrived(qin.at[level, k], q_recv.at[level, k])
                total = total - qin[level, k].astype(jnp.float32)
        result = dot_nt(total.astype(jnp.bfloat16), inverse(level))
        if level < subl:
            sol_sub[0, level, 0] = result
        else:
            sol_top[level - subl, 0] = result
        if level > 0:
            ans[level, j] = result.astype(jnp.bfloat16)
            for d in range(1, n):
                put(
                    ans.at[level, j],
                    ans.at[level, j],
                    a_send.at[level, d],
                    a_recv.at[level, j],
                    {"col": lax.rem(j + d, n)},
                )

    for copy, remote in pending:
        if remote is None:
            copy.wait_send()
        else:

            @pl.when(remote)
            def _():
                copy.wait_send()


def fused_device(*args):
    rhs_sub, rhs_top, lower_sub, lower_link, lower_top = args[:5]
    levels = rhs_sub.shape[1] + rhs_top.shape[0]
    topl = rhs_top.shape[0]
    share, width = rhs_top.shape[2:]
    n = lax.axis_size("col")
    masks = jnp.concatenate([value.reshape(-1) for value in args[7:]])
    units = lower_sub.shape[1] + lower_link.shape[1] + lower_top.shape[0]
    half, dma = jnp.bfloat16, pltpu.SemaphoreType.DMA
    vmem = pl.BlockSpec(memory_space=pltpu.VMEM)
    smem = pl.BlockSpec(memory_space=pltpu.SMEM)
    vectors = pltpu.VMEM((levels, n, share, width), half)
    return pl.pallas_call(
        fused_kernel,
        out_shape=(
            jax.ShapeDtypeStruct(rhs_sub.shape, jnp.float32),
            jax.ShapeDtypeStruct(rhs_top.shape, jnp.float32),
        ),
        in_specs=[vmem] * 7 + [smem],
        out_specs=(vmem, vmem),
        scratch_shapes=[
            pltpu.VMEM((units, width, width), half),
            pltpu.VMEM((levels, share, width), jnp.float32),
            pltpu.VMEM((levels, share, width), half),
            vectors,
            vectors,
            vectors,
            pltpu.VMEM((n, topl, share, width), half),
            pltpu.VMEM((n, topl, share, width), half),
            vectors,
            vectors,
            vectors,
            dma((levels, n)),
            dma((levels, n)),
            dma((levels, n)),
            dma((levels, n)),
            dma((n,)),
            dma((n,)),
            dma((levels, n)),
            dma((levels, n)),
            dma((levels, n)),
            dma((levels, n)),
        ],
        compiler_params=pltpu.CompilerParams(has_side_effects=True),
    )(*args[:7], masks)


def choose(*args):
    rhs_top, lower_top = args[1], args[4]
    one_each = lower_top.shape[1] == 1 and lower_top.shape[2] == 1
    square = lax.axis_size("row") == lax.axis_size("col") and lax.axis_size("gz") == 2
    if one_each and square and rhs_top.shape[2] % 8 == 0 and rhs_top.shape[3] % 128 == 0:
        return fused_device(*args)
    return per_device(*args)


def solution(mesh):
    return jax.shard_map(
        choose,
        mesh=mesh,
        in_specs=(
            P("gz", None, "row", "col", None),
            P(None, "row", "col", None),
            P("gz", None, "row", "col", None, None),
            P("gz", None, "row", "col", None, None),
            P(None, "row", "col", None, None),
            P("gz", None, "row", None, None),
            P(None, "row", None, None),
            P("gz", None, "row", "col"),
            P("gz", None, "row", "col"),
            P(None, "row", "col"),
        ),
        out_specs=(P("gz", None, "row", "col", None), P(None, "row", "col", None)),
        check_vma=False,
    )
```
